32 devices in a mesh: mem: 16 (over z, y, x), tile: 2 (over core).
Axes of the slice: x: 2, y: 2, z: 4, core: 2. Of those that a mesh axis runs over, the one named last changes fastest.
Arguments:
- starting_samples: float32 [512, 128, 256], P('mem', 'tile'), may hold values from -6 to 6
- transport_number_vertical: float32 [128, 256], P('tile'), may hold values from 0.1 to 0.35
- transport_number_horizontal: float32 [128, 256], P('tile'), may hold values from 0.1 to 0.35
- spreading_number: float32 [128, 256], P('tile'), may hold values from 0.01 to 0.07
- obs_value: float32 [2, 16, 128], P('tile'), may hold values from -6 to 6
- obs_error: float32 [2, 16, 128], P('tile'), may hold values from 0.002 to 0.05
- obs_index: int32 [2, 16, 128], P('tile'), may hold values from 0 to 1023
- loc_index: int32 [2, 16, 128], P('tile'), may hold values from 0 to 7
- loc_table: float32 [3, 8], replicated, may hold values from 0.2 to 1
Outputs:
- analysis: float32 [512, 128, 256], P('mem', 'tile')
The draws below stay inside these ranges and needn't reach their ends.
Inputs may be any that keep to these rules, and one draw needn't show every extreme that they name: Observation j of a patch lies in the patch's cell obs_index, cells numbered row by row, 16 to a row.
All inputs are finite; a program needn't handle non-finite values.
Results may differ from the reference program's by a relative error of at most 0.0003.
Values sent between devices are 32-bit elements; how exact they have to be, the bound alone decides.
No kernel may reach another device: no remote copies, remote signals or barrier semaphores. Data moves between devices by JAX's collectives and lax.ppermute only.
A program may use at most 128 MiB of HBM per device.

```python
import math
import jax
import jax.numpy as jnp
from jax import lax

ENSEMBLE_SIZE_N = 512
STRIP_HEIGHT = 64
BLOCK_WIDTH = 16
NOBS = 128
LEVELS = 8
PASSES = 6
NS_ITERS = 8
STRIP_TOTAL = 2
BLOCKS_ACROSS = 16
NX = 256
NY = 128
PATCH_CELLS = 1024


def place_ends(values, stream_key, smallest, top_value):
    index_at = [jax.random.randint(jax.random.fold_in(stream_key, axis), (), 0, length) for axis, length in enumerate(values.shape)]
    widest = values.shape.index(max(values.shape))
    next_to = index_at[:widest] + [(index_at[widest] + 1) % values.shape[widest]] + index_at[widest + 1:]
    return values.at[tuple(index_at)].set(smallest).at[tuple(next_to)].set(top_value)


def block_scale(key, dims, cuts, low, high):
    loudness = 1.0
    for axis_at, blocks in cuts:
        heights = jax.random.uniform(jax.random.fold_in(jax.random.fold_in(key, 6), axis_at), (blocks,), jnp.float32, low / len(cuts), high / len(cuts))
        loudness = loudness * jnp.repeat(jnp.exp(heights), dims[axis_at] // blocks).reshape((-1,) + (1,) * (len(dims) - 1 - axis_at))
    return loudness


def bell_draw(rng, extent, deviation, limit, split=(), kind=jnp.bfloat16):
    array = deviation * jax.random.normal(rng, extent, jnp.float32)
    if split:
        array = array * block_scale(rng, extent, split, -0.22, 0.18)
    return jnp.clip(array, -limit, limit).astype(kind)


def setup_inputs(seed: int = 0) -> dict:
    splits = jax.random.split(jax.random.key(seed), 10)
    starting_samples = bell_draw(splits[0], (ENSEMBLE_SIZE_N, NY, NX), 1.0, 6.0, ((0, 16), (1, 2)), jnp.float32)
    transport_number_vertical = jnp.clip(0.1 + 0.25 * jax.random.uniform(splits[1], (NY, NX), jnp.float32) ** block_scale(splits[1], (NY, NX), ((0, 2),), -0.2, 0.2), 0.1, 0.35)
    transport_number_horizontal = jnp.clip(0.1 + 0.25 * jax.random.uniform(splits[2], (NY, NX), jnp.float32) ** block_scale(splits[2], (NY, NX), ((0, 2),), -0.2, 0.2), 0.1, 0.35)
    spreading_number = jnp.clip(0.01 + 0.060000001 * jax.random.uniform(splits[3], (NY, NX), jnp.float32) ** block_scale(splits[3], (NY, NX), ((0, 2),), -0.2, 0.2), 0.01, 0.07)
    obs_value = bell_draw(splits[4], (STRIP_TOTAL, BLOCKS_ACROSS, NOBS), 1.0, 6.0, ((0, 2),), jnp.float32)
    obs_error = jnp.clip(jnp.exp(math.log(0.05) - 3.218876 * jax.random.uniform(splits[5], (STRIP_TOTAL, BLOCKS_ACROSS, NOBS), jnp.float32) ** block_scale(splits[5], (STRIP_TOTAL, BLOCKS_ACROSS, NOBS), ((0, 2),), -0.2, 0.2)), 0.002, 0.05)
    obs_index = place_ends(jax.random.randint(splits[6], (STRIP_TOTAL, BLOCKS_ACROSS, NOBS), 0, PATCH_CELLS), jax.random.fold_in(splits[6], 1), 0, PATCH_CELLS - 1).astype(jnp.int32)
    loc_index = place_ends(jax.random.randint(splits[7], (STRIP_TOTAL, BLOCKS_ACROSS, NOBS), 0, LEVELS), jax.random.fold_in(splits[7], 1), 0, LEVELS - 1).astype(jnp.int32)
    loc_table = jnp.clip(jnp.exp(jax.random.uniform(splits[8], (3, LEVELS), jnp.float32, math.log(0.2), math.log(1.0))), 0.2, 1.0)
    return {"starting_samples": starting_samples, "transport_number_vertical": transport_number_vertical, "transport_number_horizontal": transport_number_horizontal, "spreading_number": spreading_number, "obs_value": obs_value, "obs_error": obs_error, "obs_index": obs_index, "loc_index": loc_index, "loc_table": loc_table}


def advance(middle, northern, southern, speed_x, speed_y, mixing, roll_axis):
    western = jnp.roll(middle, 1, axis=roll_axis)
    eastern = jnp.roll(middle, -1, axis=roll_axis)
    return middle + speed_x * (western - middle) + speed_y * (northern - middle) + mixing * (northern + southern + western + eastern - 4.0 * middle)

def transform(members, observed, values, errors, levels, loc_table):
    ensemble_size = members.shape[0]
    center = lax.optimization_barrier(jnp.mean(members, axis=0))
    anomaly = members - center
    obs_mean = lax.optimization_barrier(jnp.mean(observed, axis=1))
    spread = observed - obs_mean[:, None, :]
    innovation = values - obs_mean
    onehot = (levels[:, :, None] == jnp.arange(loc_table.shape[1], dtype=jnp.int32)).astype(jnp.float32)
    weights = lax.optimization_barrier(jnp.sum(onehot * loc_table[:, None, :], axis=2))
    precision_obs = weights / errors
    stacked = jnp.transpose(spread, (1, 0, 2)).reshape(ensemble_size, -1)
    scaled_obs = precision_obs.reshape(-1)
    weighted_innov = (precision_obs * innovation).reshape(-1)
    identity = jnp.eye(ensemble_size, dtype=jnp.float32)
    gram_matrix = (ensemble_size - 1.0) * identity + jnp.dot(stacked * scaled_obs, stacked.T, precision=lax.Precision.HIGHEST)
    norm_scale = jnp.sqrt(jnp.sum(gram_matrix * gram_matrix))
    matrix = gram_matrix / norm_scale
    inverse_root = identity
    for repeat in range(NS_ITERS):
        factor = 1.5 * identity - 0.5 * jnp.dot(inverse_root, matrix, precision=lax.Precision.HIGHEST)
        matrix = jnp.dot(matrix, factor, precision=lax.Precision.HIGHEST)
        inverse_root = jnp.dot(factor, inverse_root, precision=lax.Precision.HIGHEST)
    obs_pull = jnp.dot(stacked, weighted_innov, precision=lax.Precision.HIGHEST)
    mean_weight = jnp.dot(inverse_root, jnp.dot(inverse_root, obs_pull, precision=lax.Precision.HIGHEST), precision=lax.Precision.HIGHEST) / norm_scale
    weight = jnp.sqrt((ensemble_size - 1.0) / norm_scale) * inverse_root + mean_weight[:, None]
    return center + jnp.dot(weight.T, anomaly, precision=lax.Precision.HIGHEST)

def sample_prediction(model_mesh_values, transport_number_vertical, transport_number_horizontal, spreading_number):
    for repeat in range(PASSES):
        northern = jnp.roll(model_mesh_values, 1, axis=0)
        southern = jnp.roll(model_mesh_values, -1, axis=0)
        model_mesh_values = advance(model_mesh_values, northern, southern, transport_number_vertical, transport_number_horizontal, spreading_number, 1)
    return model_mesh_values

def reference(starting_samples, transport_number_vertical, transport_number_horizontal, spreading_number, obs_value, obs_error, obs_index, loc_index, loc_table):
    predict_advance = lax.map(lambda sample_mesh_values: sample_prediction(sample_mesh_values, transport_number_vertical, transport_number_horizontal, spreading_number), starting_samples)
    row_in = obs_index // BLOCK_WIDTH
    col_in = obs_index % BLOCK_WIDTH
    entire_mesh_lines = jnp.arange(STRIP_TOTAL, dtype=jnp.int32)[:, None, None] * STRIP_HEIGHT + row_in
    domain_verticals = jnp.arange(BLOCKS_ACROSS, dtype=jnp.int32)[None, :, None] * BLOCK_WIDTH + col_in
    measured_at_all_sites = predict_advance[:, entire_mesh_lines, domain_verticals]
    block_sequence = predict_advance.reshape(ENSEMBLE_SIZE_N, STRIP_TOTAL, STRIP_HEIGHT, BLOCKS_ACROSS, BLOCK_WIDTH)
    zero_index = jnp.zeros((), jnp.int32)

    def one_patch(flat_index):
        tile_number = (flat_index // BLOCKS_ACROSS).astype(jnp.int32)
        block_number = (flat_index % BLOCKS_ACROSS).astype(jnp.int32)
        members = lax.dynamic_slice(block_sequence, (zero_index, tile_number, zero_index, block_number, zero_index), (ENSEMBLE_SIZE_N, 1, STRIP_HEIGHT, 1, BLOCK_WIDTH)).reshape(ENSEMBLE_SIZE_N, STRIP_HEIGHT * BLOCK_WIDTH)
        role_blocks = (block_number + jnp.arange(3, dtype=jnp.int32) - 1) % BLOCKS_ACROSS
        seen_values = jnp.transpose(measured_at_all_sites[:, tile_number][:, role_blocks], (1, 0, 2))
        values = obs_value[tile_number][role_blocks]
        errors = obs_error[tile_number][role_blocks]
        levels = loc_index[tile_number][role_blocks]
        return transform(members, seen_values, values, errors, levels, loc_table)
    result = lax.map(one_patch, jnp.arange(STRIP_TOTAL * BLOCKS_ACROSS, dtype=jnp.int32))
    result = result.reshape(STRIP_TOTAL, BLOCKS_ACROSS, ENSEMBLE_SIZE_N, STRIP_HEIGHT, BLOCK_WIDTH)
    return jnp.transpose(result, (2, 0, 3, 1, 4)).reshape(ENSEMBLE_SIZE_N, NY, NX)
```

```python
import functools

import jax
import jax.numpy as jnp
from jax import lax
from jax.experimental import pallas as pl
from jax.experimental.pallas import tpu as pltpu
from jax.sharding import PartitionSpec as P

PASSES = 6
NS_ITERS = 8
HALO = 8
F32 = jnp.float32
BF16 = jnp.bfloat16
VMEM = pl.BlockSpec(memory_space=pltpu.VMEM)
SMEM = pl.BlockSpec(memory_space=pltpu.SMEM)


def split(x):
    high = x.astype(BF16)
    return high, (x - high.astype(F32)).astype(BF16)


def dot_split(a, b, dims=(((1,), (0,)), ((), ()))):
    (ah, al), (bh, bl) = a, b
    dot = functools.partial(lax.dot_general, dimension_numbers=dims, preferred_element_type=F32)
    return dot(ah, bh) + (dot(ah, bl) + dot(al, bh))


def swap_granules(rows, lane, width):
    count = len(rows)
    rows = list(rows)
    step = count // 2
    while step:
        odd = (lane // (width * step)) % 2 == 1
        for i in range(count):
            if i & step:
                continue
            a, b = rows[i], rows[i + step]
            rows[i] = jnp.where(odd, pltpu.roll(b, width * step, axis=1), a)
            rows[i + step] = jnp.where(odd, b, pltpu.roll(a, 128 - width * step, axis=1))
        step //= 2
    return rows


def forecast_kernel(blocks, patch_ref, x_ref, up_ref, down_ref, av_ref, ah_ref, sp_ref, index_ref, *rest):
    outs, seen = rest[:blocks], rest[blocks : 2 * blocks]
    one, two, coef, fields = rest[2 * blocks :]
    members, rows, columns = x_ref.shape
    total = rows + 2 * HALO
    width = columns // blocks
    per = 128 // width
    cells = rows * width

    def place(source, member, row, target):
        tile = source[pl.ds(member, 8), pl.ds(row, 8), :]
        one[pl.ds(target, 8), pl.ds(member, 8), :] = jnp.swapaxes(tile, 0, 1)

    def load_rows(t, carry):
        row = pl.multiple_of(t * 8, 8)
        for m in range(0, members, 8):
            place(x_ref, m, row, HALO + row)
        return carry

    lax.fori_loop(0, rows // 8, load_rows, 0)
    for m in range(0, members, 8):
        place(up_ref, m, 0, 0)
        place(down_ref, m, 0, HALO + rows)

    def spread_coef(av, ah, sp, target):
        for n, value in enumerate((1.0 - av - ah - 4.0 * sp, av + sp, ah + sp, sp)):
            for i in range(8):
                coef[n, target + i] = jnp.broadcast_to(value[i : i + 1], (8, columns))

    spread_coef(up_ref[members], up_ref[members + 1], up_ref[members + 2], 0)
    spread_coef(down_ref[members], down_ref[members + 1], down_ref[members + 2], HALO + rows)

    def coef_rows(t, carry):
        row = pl.multiple_of(t * 8, 8)
        spread_coef(av_ref[pl.ds(row, 8), :], ah_ref[pl.ds(row, 8), :], sp_ref[pl.ds(row, 8), :], HALO + row)
        return carry

    lax.fori_loop(0, rows // 8, coef_rows, 0)

    def wide(value):
        return jnp.concatenate([value] * (members // 8), axis=0)

    buffers = (one, two)
    for step in range(1, PASSES + 1):
        source, target = buffers[(step - 1) % 2], buffers[step % 2]
        first = HALO - PASSES + step
        count = total - 2 * first

        def advance(t, carry, source=source, target=target, first=first):
            row = first + 2 * t
            lines = [source[row - 1 + i] for i in range(4)]
            for i in range(2):
                north, middle, south = lines[i : i + 3]
                west = pltpu.roll(middle, 1, axis=1)
                east = pltpu.roll(middle, columns - 1, axis=1)
                target[row + i] = (
                    wide(coef[0, row + i]) * middle
                    + wide(coef[1, row + i]) * west
                    + wide(coef[2, row + i]) * north
                    + wide(coef[3, row + i]) * (south + east)
                )
            return carry

        lax.fori_loop(0, count // 2, advance, 0)

    final = buffers[PASSES % 2]
    lane = lax.broadcasted_iota(jnp.int32, (members, 128), 1)

    def cut(t, carry):
        row = HALO + t * per
        at = pl.multiple_of(t * 128, 128)
        for h in range(columns // 128):
            lines = [final[row + i, :, h * 128 : (h + 1) * 128] for i in range(per)]
            for j, piece in enumerate(swap_granules(lines, lane, width)):
                fields[h * per + j, :, pl.ds(at, 128)] = piece
        return carry

    lax.fori_loop(0, rows // per, cut, 0)
    for k in range(blocks):
        patch = patch_ref[k]
        index = jnp.broadcast_to(index_ref[patch], (members, 128))
        low, high = index % 128, index // 128
        value = jnp.zeros((members, 128), F32)
        for t in range(cells // 128):
            part = fields[patch, :, t * 128 : (t + 1) * 128]
            outs[k][:, t * 128 : (t + 1) * 128] = part
            picked = jnp.take_along_axis(part, low, axis=1, mode="promise_in_bounds")
            value = jnp.where(high == t, picked, value)
        seen[k][...] = value


def weight_kernel(blocks, shift_ref, own_ref, left_ref, right_ref, prec_ref, value_ref, high_ref, low_ref, stacked, mh, ml, zh, zl, fh, fl):
    size, nobs = own_ref.shape[0] * own_ref.shape[1], own_ref.shape[2]
    chunk = own_ref.shape[1]
    for role, ref in enumerate((left_ref, own_ref, right_ref)):
        for k in range(blocks):
            piece = ref[k] if role == 1 else ref[jnp.bitwise_xor(shift_ref[role], k)]
            stacked[k * chunk : (k + 1) * chunk, role * nobs : (role + 1) * nobs] = piece
    mean = jnp.sum(stacked[...], axis=0, keepdims=True) * (1.0 / size)
    stacked[...] = stacked[...] - mean
    prec = prec_ref[...]
    spread = stacked[...]
    pull = jnp.sum(spread * (prec * (value_ref[...] - mean)), axis=1, keepdims=True)
    contract = (((1,), (1,)), ((), ()))
    gram = dot_split(split(spread * prec), split(spread), contract)
    eye = lax.broadcasted_iota(jnp.int32, (size, size), 0) == lax.broadcasted_iota(jnp.int32, (size, size), 1)
    gram = gram + jnp.where(eye, size - 1.0, 0.0)
    total = jnp.sum(jnp.sum(gram * gram, axis=0, keepdims=True), axis=1, keepdims=True)
    scale = lax.rsqrt(total)
    norm = jnp.sqrt(total)
    matrix = gram / norm

    def factor_of(product):
        diagonal = lax.broadcasted_iota(jnp.int32, (size, size), 0) == lax.broadcasted_iota(jnp.int32, (size, size), 1)
        return jnp.where(diagonal, 1.5, 0.0) - 0.5 * product

    mh[...], ml[...] = split(matrix)
    fh[...], fl[...] = split(factor_of(matrix))
    zh[...], zl[...] = fh[...], fl[...]
    mh[...], ml[...] = split(dot_split((mh[...], ml[...]), (fh[...], fl[...])))

    def iterate(step, carry):
        fh[...], fl[...] = split(factor_of(dot_split((zh[...], zl[...]), (mh[...], ml[...]))))
        mh[...], ml[...] = split(dot_split((mh[...], ml[...]), (fh[...], fl[...])))
        zh[...], zl[...] = split(dot_split((fh[...], fl[...]), (zh[...], zl[...])))
        return carry

    lax.fori_loop(0, NS_ITERS - 2, iterate, 0)
    fh[...], fl[...] = split(factor_of(dot_split((zh[...], zl[...]), (mh[...], ml[...]))))
    root = dot_split((fh[...], fl[...]), (zh[...], zl[...]))
    once = jnp.sum(root * pull, axis=0, keepdims=True)
    twice = jnp.sum(root * once, axis=1, keepdims=True) / norm
    weight = jnp.sqrt((size - 1.0) * scale) * root + twice
    high_ref[...], low_ref[...] = split(weight)


def analysis_kernel(blocks, high_ref, low_ref, *rest):
    fields, outs = rest[:blocks], rest[blocks : 2 * blocks]
    ah, al, center = rest[2 * blocks :]
    chunk = fields[0].shape[0]
    size = blocks * chunk
    total = fields[0][...]
    for k in range(1, blocks):
        total = total + fields[k][...]
    center[...] = jnp.sum(total, axis=0, keepdims=True) * (1.0 / size)
    for k in range(blocks):
        high, low = split(fields[k][...] - center[...])
        ah[k * chunk : (k + 1) * chunk, :] = high
        al[k * chunk : (k + 1) * chunk, :] = low
    contract = (((0,), (0,)), ((), ()))
    result = dot_split((high_ref[...], low_ref[...]), (ah[...], al[...]), contract)
    for k in range(blocks):
        outs[k][...] = center[...] + result[k * chunk : (k + 1) * chunk, :]


def assemble_kernel(blocks, patch_ref, *rest):
    pieces, out_ref = rest[:blocks], rest[blocks]
    fields, lines_ref = rest[blocks + 1 :]
    members, rows, columns = out_ref.shape
    width = columns // blocks
    per = 128 // width
    for k in range(blocks):
        fields[patch_ref[k]] = pieces[k][...]
    lane = lax.broadcasted_iota(jnp.int32, (members, 128), 1)

    def join(t, carry):
        at = pl.multiple_of(t * 128, 128)
        for h in range(columns // 128):
            granules = [fields[h * per + j, :, pl.ds(at, 128)] for j in range(per)]
            for i, line in enumerate(swap_granules(granules, lane, width)):
                lines_ref[i, :, h * 128 : (h + 1) * 128] = line
        row = pl.multiple_of(t * per, 8)
        for m in range(0, members, 8):
            tile = lines_ref[:, m : m + 8, :]
            out_ref[m : m + 8, pl.ds(row, 8), :] = jnp.swapaxes(tile, 0, 1)
        return carry

    lax.fori_loop(0, rows // per, join, 0)


def cost(flops, moved):
    return pl.CostEstimate(flops=int(flops), bytes_accessed=int(moved), transcendentals=0)


def shape(dims, dtype=F32):
    return jax.ShapeDtypeStruct(dims, dtype)


PARAMS = pltpu.CompilerParams(vmem_limit_bytes=56 * 1024 * 1024)


def body(
    starting_samples,
    transport_number_vertical,
    transport_number_horizontal,
    spreading_number,
    obs_value,
    obs_error,
    obs_index,
    loc_index,
    loc_table,
):
    blocks = lax.axis_size("mem")
    tiles = lax.axis_size("tile")
    members, rows, columns = starting_samples.shape
    nobs = obs_index.shape[2]
    cells = rows * (columns // blocks)
    size = blocks * members
    me = lax.axis_index("mem")

    packed = jnp.concatenate(
        [starting_samples, jnp.stack([transport_number_vertical, transport_number_horizontal, spreading_number])],
        axis=0,
    ) if False else None
    coefs = (transport_number_vertical, transport_number_horizontal, spreading_number)

    def edge(part):
        return jnp.concatenate([starting_samples[:, part]] + [c[None, part] for c in coefs], axis=0)

    up = [(i, (i + 1) % tiles) for i in range(tiles)]
    down = [(j, i) for i, j in up]
    above = lax.ppermute(edge(slice(rows - HALO, rows)), "tile", up)
    below = lax.ppermute(edge(slice(0, HALO)), "tile", down)

    patches = jnp.bitwise_xor(me, jnp.arange(blocks, dtype=jnp.int32))
    results = pl.pallas_call(
        functools.partial(forecast_kernel, blocks),
        out_shape=[shape((members, cells))] * blocks + [shape((members, nobs))] * blocks,
        in_specs=[SMEM] + [VMEM] * 7,
        out_specs=[VMEM] * (2 * blocks),
        scratch_shapes=[
            pltpu.VMEM((rows + 2 * HALO, members, columns), F32),
            pltpu.VMEM((rows + 2 * HALO, members, columns), F32),
            pltpu.VMEM((4, rows + 2 * HALO, 8, columns), F32),
            pltpu.VMEM((blocks, members, cells), F32),
        ],
        compiler_params=PARAMS,
        cost_estimate=cost(5e6, 5e6),
        name="forecast",
    )(patches, starting_samples, above, below, *coefs, obs_index[0][:, None, :])
    fields, seen = results[:blocks], results[blocks:]

    def swap(x, k):
        return lax.ppermute(x, "mem", [(i, i ^ k) for i in range(blocks)])

    order = sorted(range(1, blocks), reverse=True)
    seen = [seen[0]] + [swap(seen[k], k) for k in range(1, blocks)]
    fields_in = {0: fields[0]}
    for k in order:
        fields_in[k] = swap(fields[k], k)
    own = jnp.stack(seen, axis=0)
    ring = [(i, (i + 1) % blocks) for i in range(blocks)]
    left = lax.ppermute(own, "mem", ring)
    right = lax.ppermute(own, "mem", [(j, i) for i, j in ring])

    roles = (me + jnp.arange(3, dtype=jnp.int32) - 1) % blocks
    onehot = (loc_index[0][roles][:, :, None] == jnp.arange(loc_table.shape[1], dtype=jnp.int32)).astype(F32)
    precision = jnp.sum(onehot * loc_table[:, None, :], axis=2) / obs_error[0][roles]
    values = obs_value[0][roles]
    shift = jnp.bitwise_xor(me, roles)
    high, low = pl.pallas_call(
        functools.partial(weight_kernel, blocks),
        out_shape=[shape((size, size), BF16)] * 2,
        in_specs=[SMEM] + [VMEM] * 5,
        out_specs=[VMEM] * 2,
        scratch_shapes=[pltpu.VMEM((size, 3 * nobs), F32)] + [pltpu.VMEM((size, size), BF16)] * 6,
        compiler_params=PARAMS,
        cost_estimate=cost(5e9, 5e6),
        name="weight",
    )(shift, own, left, right, precision.reshape(1, -1), values.reshape(1, -1))

    results = pl.pallas_call(
        functools.partial(analysis_kernel, blocks),
        out_shape=[shape((members, cells))] * blocks,
        in_specs=[VMEM] * (2 + blocks),
        out_specs=[VMEM] * blocks,
        scratch_shapes=[pltpu.VMEM((size, cells), BF16)] * 2 + [pltpu.VMEM((1, cells), F32)],
        compiler_params=PARAMS,
        cost_estimate=cost(1e9, 5e6),
        name="analysis",
    )(high, low, *[fields_in[k] for k in range(blocks)])

    back = {0: results[0]}
    for k in order:
        back[k] = swap(results[k], k)
    return pl.pallas_call(
        functools.partial(assemble_kernel, blocks),
        out_shape=shape((members, rows, columns)),
        in_specs=[SMEM] + [VMEM] * blocks,
        out_specs=VMEM,
        scratch_shapes=[pltpu.VMEM((blocks, members, cells), F32), pltpu.VMEM((8, members, columns), F32)],
        compiler_params=PARAMS,
        cost_estimate=cost(1e6, 5e6),
        name="assemble",
    )(patches, *[back[k] for k in range(blocks)])


def solution(mesh):
    in_specs = (
        P("mem", "tile", None),
        P("tile", None),
        P("tile", None),
        P("tile", None),
        P("tile", None, None),
        P("tile", None, None),
        P("tile", None, None),
        P("tile", None, None),
        P(),
    )
    out_specs = P("mem", "tile", None)
    return jax.shard_map(body, mesh=mesh, in_specs=in_specs, out_specs=out_specs, check_vma=False)
```

```python
import functools

import jax
import jax.numpy as jnp
from jax import lax
from jax.experimental import pallas as pl
from jax.experimental.pallas import tpu as pltpu
from jax.sharding import PartitionSpec as P


PASSES = 6
NS_ITERS = 8
HALO = 8
LINES = 16
F32 = jnp.float32
BF16 = jnp.bfloat16
VMEM = pl.BlockSpec(memory_space=pltpu.VMEM)
SMEM = pl.BlockSpec(memory_space=pltpu.SMEM)


def split(x):
    high = x.astype(BF16)
    return high, (x - high.astype(F32)).astype(BF16)


def dot_split(a, b, dims=(((1,), (0,)), ((), ()))):
    (ah, al), (bh, bl) = a, b
    dot = functools.partial(lax.dot_general, dimension_numbers=dims, preferred_element_type=F32)
    return dot(ah, bh) + (dot(ah, bl) + dot(al, bh))


def swap_granules(rows, lane, width):
    count = len(rows)
    rows = list(rows)
    step = count // 2
    while step:
        odd = (lane // (width * step)) % 2 == 1
        for i in range(count):
            if i & step:
                continue
            a, b = rows[i], rows[i + step]
            rows[i] = jnp.where(odd, pltpu.roll(b, width * step, axis=1), a)
            rows[i + step] = jnp.where(odd, b, pltpu.roll(a, 128 - width * step, axis=1))
        step //= 2
    return rows


def forecast_kernel(blocks, x_ref, up_ref, down_ref, av_ref, ah_ref, sp_ref, index_ref, fields, seen, one, two, coef):
    members, rows, columns = x_ref.shape
    total = rows + 2 * HALO
    width = columns // blocks
    per = 128 // width
    cells = rows * width

    def place(source, member, row, target):
        tile = source[pl.ds(member, 8), pl.ds(row, 8), :]
        one[pl.ds(target, 8), pl.ds(member, 8), :] = jnp.swapaxes(tile, 0, 1)

    def load_rows(t, carry):
        row = pl.multiple_of(t * 8, 8)
        for m in range(0, members, 8):
            place(x_ref, m, row, HALO + row)
        return carry

    lax.fori_loop(0, rows // 8, load_rows, 0)
    for m in range(0, members, 8):
        place(up_ref, m, 0, 0)
        place(down_ref, m, 0, HALO + rows)

    def spread_coef(av, ah, sp, target):
        for n, value in enumerate((1.0 - av - ah - 4.0 * sp, av + sp, ah + sp, sp)):
            for i in range(8):
                coef[n, target + i] = jnp.broadcast_to(value[i : i + 1], (8, columns))

    spread_coef(up_ref[members], up_ref[members + 1], up_ref[members + 2], 0)
    spread_coef(down_ref[members], down_ref[members + 1], down_ref[members + 2], HALO + rows)

    def coef_rows(t, carry):
        row = pl.multiple_of(t * 8, 8)
        spread_coef(av_ref[pl.ds(row, 8), :], ah_ref[pl.ds(row, 8), :], sp_ref[pl.ds(row, 8), :], HALO + row)
        return carry

    lax.fori_loop(0, rows // 8, coef_rows, 0)

    def wide(value):
        return jnp.concatenate([value] * (members // 8), axis=0)

    buffers = (one, two)
    for step in range(1, PASSES + 1):
        source, target = buffers[(step - 1) % 2], buffers[step % 2]
        first = HALO - PASSES + step
        count = total - 2 * first

        def advance(row, lines, source=source, target=target):
            middle = [source[row + i] for i in range(-1, lines + 1)]
            west = [pltpu.roll(m, 1, axis=1) for m in middle[1:-1]]
            east = [pltpu.roll(m, columns - 1, axis=1) for m in middle[1:-1]]
            for i in range(lines):
                target[row + i] = (
                    wide(coef[0, row + i]) * middle[i + 1]
                    + wide(coef[2, row + i]) * middle[i]
                    + wide(coef[1, row + i]) * west[i]
                    + wide(coef[3, row + i]) * (middle[i + 2] + east[i])
                )

        def sweep(t, carry, first=first, advance=advance):
            advance(first + LINES * t, LINES)
            return carry

        lax.fori_loop(0, count // LINES, sweep, 0)
        if count % LINES:
            advance(first + count // LINES * LINES, count % LINES)

    final = buffers[PASSES % 2]
    lane = lax.broadcasted_iota(jnp.int32, (members, 128), 1)

    def cut(t, carry):
        row = HALO + t * per
        at = pl.multiple_of(t * 128, 128)
        for h in range(columns // 128):
            lines = [final[row + i, :, h * 128 : (h + 1) * 128] for i in range(per)]
            for j, piece in enumerate(swap_granules(lines, lane, width)):
                fields[h * per + j, :, pl.ds(at, 128)] = piece
        return carry

    lax.fori_loop(0, rows // per, cut, 0)

    def look(b, carry):
        index = jnp.broadcast_to(index_ref[b], (members, 128))
        low, high = index % 128, index // 128
        value = jnp.zeros((members, 128), F32)
        for t in range(cells // 128):
            part = fields[b, :, t * 128 : (t + 1) * 128]
            picked = jnp.take_along_axis(part, low, axis=1, mode="promise_in_bounds")
            value = jnp.where(high == t, picked, value)
        seen[b] = value
        return carry

    lax.fori_loop(0, blocks, look, 0)


def weight_kernel(partner_ref, own_ref, left_ref, right_ref, prec_ref, value_ref, high_ref, low_ref, stacked, innovation, mh, ml, zh, zl, fh, fl):
    blocks, chunk, nobs = own_ref.shape
    size = blocks * chunk
    for role, ref in enumerate((left_ref, own_ref, right_ref)):
        piece = ref[...].reshape(size, nobs)
        mean = jnp.sum(piece, axis=0, keepdims=True) * (1.0 / size)
        stacked[:, role * nobs : (role + 1) * nobs] = piece - mean
        innovation[:, role * nobs : (role + 1) * nobs] = value_ref[:, role * nobs : (role + 1) * nobs] - mean
    prec = prec_ref[...]
    spread = stacked[...]
    pull = jnp.sum(spread * (prec * innovation[...]), axis=1, keepdims=True)
    contract = (((1,), (1,)), ((), ()))
    gram = dot_split(split(spread * prec), split(spread), contract)
    eye = lax.broadcasted_iota(jnp.int32, (size, size), 0) == lax.broadcasted_iota(jnp.int32, (size, size), 1)
    gram = gram + jnp.where(eye, size - 1.0, 0.0)
    total = jnp.sum(jnp.sum(gram * gram, axis=0, keepdims=True), axis=1, keepdims=True)
    scale = lax.rsqrt(total)
    norm = jnp.sqrt(total)
    matrix = gram / norm

    def factor_of(product):
        diagonal = lax.broadcasted_iota(jnp.int32, (size, size), 0) == lax.broadcasted_iota(jnp.int32, (size, size), 1)
        return jnp.where(diagonal, 1.5, 0.0) - 0.5 * product

    mh[...], ml[...] = split(matrix)
    fh[...], fl[...] = split(factor_of(matrix))
    zh[...], zl[...] = fh[...], fl[...]
    mh[...], ml[...] = split(dot_split((mh[...], ml[...]), (fh[...], fl[...])))

    def iterate(step, carry):
        fh[...], fl[...] = split(factor_of(dot_split((zh[...], zl[...]), (mh[...], ml[...]))))
        mh[...], ml[...] = split(dot_split((mh[...], ml[...]), (fh[...], fl[...])))
        zh[...], zl[...] = split(dot_split((fh[...], fl[...]), (zh[...], zl[...])))
        return carry

    lax.fori_loop(0, NS_ITERS - 2, iterate, 0)
    fh[...], fl[...] = split(factor_of(dot_split((zh[...], zl[...]), (mh[...], ml[...]))))
    root = dot_split((fh[...], fl[...]), (zh[...], zl[...]))
    line = jnp.transpose(jnp.broadcast_to(pull, (size, 128)))[0:1]
    once = jnp.sum(root * line, axis=1, keepdims=True)
    twice = jnp.sum(root * once, axis=0, keepdims=True) / norm
    fh[...], fl[...] = split(jnp.sqrt((size - 1.0) * scale) * root + twice)
    for k in range(blocks):
        row = pl.multiple_of(partner_ref[k] * chunk, chunk)
        high_ref[k * chunk : (k + 1) * chunk, :] = fh[pl.ds(row, chunk), :]
        low_ref[k * chunk : (k + 1) * chunk, :] = fl[pl.ds(row, chunk), :]


def analysis_kernel(high_ref, low_ref, fields, *rest):
    outs, (ah, al, center) = rest[:-3], rest[-3:]
    blocks, chunk, _ = fields.shape
    size = blocks * chunk
    total = fields[0]
    for k in range(1, blocks):
        total = total + fields[k]
    center[...] = jnp.sum(total, axis=0, keepdims=True) * (1.0 / size)
    for k in range(blocks):
        high, low = split(fields[k] - center[...])
        ah[k * chunk : (k + 1) * chunk, :] = high
        al[k * chunk : (k + 1) * chunk, :] = low
    result = dot_split((high_ref[...], low_ref[...]), (ah[...], al[...]))
    for k in range(blocks):
        outs[k][...] = result[k * chunk : (k + 1) * chunk, :] + center[...]


def assemble_kernel(blocks, partner_ref, *rest):
    pieces, (out_ref, fields, lines_ref) = rest[:blocks], rest[blocks:]
    members, rows, columns = out_ref.shape
    for k in range(blocks):
        fields[partner_ref[k]] = pieces[k][...]
    width = columns // blocks
    per = 128 // width
    lane = lax.broadcasted_iota(jnp.int32, (members, 128), 1)

    def join(t, carry):
        at = pl.multiple_of(t * 128, 128)
        for h in range(columns // 128):
            granules = [fields[h * per + j, :, pl.ds(at, 128)] for j in range(per)]
            for i, line in enumerate(swap_granules(granules, lane, width)):
                lines_ref[i, :, h * 128 : (h + 1) * 128] = line
        row = pl.multiple_of(t * per, 8)
        for m in range(0, members, 8):
            tile = lines_ref[:, m : m + 8, :]
            out_ref[m : m + 8, pl.ds(row, 8), :] = jnp.swapaxes(tile, 0, 1)
        return carry

    lax.fori_loop(0, rows // per, join, 0)


def cost(flops, moved):
    return pl.CostEstimate(flops=int(flops), bytes_accessed=int(moved), transcendentals=0)


def shape(dims, dtype=F32):
    return jax.ShapeDtypeStruct(dims, dtype)


PARAMS = pltpu.CompilerParams(vmem_limit_bytes=56 * 1024 * 1024)


def body(
    starting_samples,
    transport_number_vertical,
    transport_number_horizontal,
    spreading_number,
    obs_value,
    obs_error,
    obs_index,
    loc_index,
    loc_table,
):
    blocks = lax.axis_size("mem")
    tiles = lax.axis_size("tile")
    members, rows, columns = starting_samples.shape
    nobs = obs_index.shape[2]
    cells = rows * (columns // blocks)
    size = blocks * members
    me = lax.axis_index("mem")

    coefs = (transport_number_vertical, transport_number_horizontal, spreading_number)

    def edge(part):
        return jnp.concatenate([starting_samples[:, part]] + [c[None, part] for c in coefs], axis=0)

    up = [(i, (i + 1) % tiles) for i in range(tiles)]
    down = [(j, i) for i, j in up]
    above = lax.ppermute(edge(slice(rows - HALO, rows)), "tile", up)
    below = lax.ppermute(edge(slice(0, HALO)), "tile", down)

    fields, seen = pl.pallas_call(
        functools.partial(forecast_kernel, blocks),
        out_shape=[shape((blocks, members, cells)), shape((blocks, members, nobs))],
        in_specs=[VMEM] * 7,
        out_specs=[VMEM] * 2,
        scratch_shapes=[
            pltpu.VMEM((rows + 2 * HALO, members, columns), F32),
            pltpu.VMEM((rows + 2 * HALO, members, columns), F32),
            pltpu.VMEM((4, rows + 2 * HALO, 8, columns), F32),
        ],
        compiler_params=PARAMS,
        cost_estimate=cost(5e6, 5e6),
        name="forecast",
    )(starting_samples, above, below, *coefs, obs_index[0][:, None, :])

    seen, obs_value, obs_error, loc_index = lax.optimization_barrier((seen, obs_value, obs_error, loc_index))
    own = lax.all_to_all(seen, "mem", 0, 0)
    roles = (me + jnp.arange(3, dtype=jnp.int32) - 1) % blocks
    onehot = (loc_index[0][roles][:, :, None] == jnp.arange(loc_table.shape[1], dtype=jnp.int32)).astype(F32)
    precision = jnp.sum(onehot * loc_table[:, None, :], axis=2) / obs_error[0][roles]
    values = obs_value[0][roles]
    partner = jnp.bitwise_xor(me, jnp.arange(blocks, dtype=jnp.int32))
    own, precision, values, partner = lax.optimization_barrier((own, precision, values, partner))
    ring = [(i, (i + 1) % blocks) for i in range(blocks)]
    left = lax.ppermute(own, "mem", ring)
    right = lax.ppermute(own, "mem", [(j, i) for i, j in ring])
    fields = lax.all_to_all(fields, "mem", 0, 0)

    high, low = pl.pallas_call(
        weight_kernel,
        out_shape=[shape((size, size), BF16)] * 2,
        in_specs=[SMEM] + [VMEM] * 5,
        out_specs=[VMEM] * 2,
        scratch_shapes=[pltpu.VMEM((size, 3 * nobs), F32), pltpu.VMEM((1, 3 * nobs), F32)]
        + [pltpu.VMEM((size, size), BF16)] * 6,
        compiler_params=PARAMS,
        cost_estimate=cost(5e9, 5e6),
        name="weight",
    )(partner, own, left, right, precision.reshape(1, -1), values.reshape(1, -1))

    result = pl.pallas_call(
        analysis_kernel,
        out_shape=[shape((members, cells))] * blocks,
        in_specs=[VMEM] * 3,
        out_specs=[VMEM] * blocks,
        scratch_shapes=[pltpu.VMEM((size, cells), BF16)] * 2 + [pltpu.VMEM((1, cells), F32)],
        compiler_params=PARAMS,
        cost_estimate=cost(1e9, 5e6),
        name="analysis",
    )(high, low, fields)

    back = {0: result[0]}
    for k in sorted(range(1, blocks), reverse=True):
        back[k] = lax.ppermute(result[k], "mem", [(i, i ^ k) for i in range(blocks)])
    return pl.pallas_call(
        functools.partial(assemble_kernel, blocks),
        out_shape=shape((members, rows, columns)),
        in_specs=[SMEM] + [VMEM] * blocks,
        out_specs=VMEM,
        scratch_shapes=[pltpu.VMEM((blocks, members, cells), F32), pltpu.VMEM((8, members, columns), F32)],
        compiler_params=PARAMS,
        cost_estimate=cost(1e6, 5e6),
        name="assemble",
    )(partner, *[back[k] for k in range(blocks)])


def solution(mesh):
    in_specs = (
        P("mem", "tile", None),
        P("tile", None),
        P("tile", None),
        P("tile", None),
        P("tile", None, None),
        P("tile", None, None),
        P("tile", None, None),
        P("tile", None, None),
        P(),
    )
    out_specs = P("mem", "tile", None)
    return jax.shard_map(body, mesh=mesh, in_specs=in_specs, out_specs=out_specs, check_vma=False)
```

```python
import functools

import jax
import jax.numpy as jnp
from jax import lax
from jax.experimental import pallas as pl
from jax.experimental.pallas import tpu as pltpu
from jax.sharding import PartitionSpec as P


PASSES = 6
NS_ITERS = 8
HALO = 8
LINES = 36
PARTS = 2
F32 = jnp.float32
BF16 = jnp.bfloat16
VMEM = pl.BlockSpec(memory_space=pltpu.VMEM)
SMEM = pl.BlockSpec(memory_space=pltpu.SMEM)
HBM = pl.BlockSpec(memory_space=pltpu.HBM)


def split(x):
    high = x.astype(BF16)
    return high, (x - high.astype(F32)).astype(BF16)


def dot_split(a, b, dims=(((1,), (0,)), ((), ()))):
    (ah, al), (bh, bl) = a, b
    dot = functools.partial(lax.dot_general, dimension_numbers=dims, preferred_element_type=F32)
    return dot(ah, bh) + (dot(ah, bl) + dot(al, bh))


def swap_granules(rows, lane, width):
    count = len(rows)
    rows = list(rows)
    step = count // 2
    while step:
        odd = (lane // (width * step)) % 2 == 1
        for i in range(count):
            if i & step:
                continue
            a, b = rows[i], rows[i + step]
            rows[i] = jnp.where(odd, pltpu.roll(b, width * step, axis=1), a)
            rows[i + step] = jnp.where(odd, b, pltpu.roll(a, 128 - width * step, axis=1))
        step //= 2
    return rows


def forecast_kernel(x_hbm, up_ref, down_ref, av_ref, ah_ref, sp_ref, index_ref, *rest):
    out, seen, x_ref, fields, one, two, coef, in_sems, out_sem = rest
    blocks = fields.shape[0]
    members, rows, columns = x_ref.shape
    loads = []
    for m in range(0, members, 8):
        loads.append(pltpu.make_async_copy(x_hbm.at[pl.ds(m, 8)], x_ref.at[pl.ds(m, 8)], in_sems.at[m // 8]))
        loads[-1].start()
    total = rows + 2 * HALO
    width = columns // blocks
    per = 128 // width
    cells = rows * width

    def place(source, member, row, target):
        tile = source[pl.ds(member, 8), pl.ds(row, 8), :]
        one[pl.ds(target, 8), pl.ds(member, 8), :] = jnp.swapaxes(tile, 0, 1)

    for m in range(0, members, 8):
        place(up_ref, m, 0, 0)
        place(down_ref, m, 0, HALO + rows)

    def spread_coef(av, ah, sp, target):
        for n, value in enumerate((1.0 - av - ah - 4.0 * sp, av + sp, ah + sp, sp)):
            for i in range(8):
                coef[n, target + i] = jnp.broadcast_to(value[i : i + 1], (8, columns))

    spread_coef(up_ref[members], up_ref[members + 1], up_ref[members + 2], 0)
    spread_coef(down_ref[members], down_ref[members + 1], down_ref[members + 2], HALO + rows)

    def coef_rows(t, carry):
        row = pl.multiple_of(t * 8, 8)
        spread_coef(av_ref[pl.ds(row, 8), :], ah_ref[pl.ds(row, 8), :], sp_ref[pl.ds(row, 8), :], HALO + row)
        return carry

    lax.fori_loop(0, rows // 8, coef_rows, 0)
    for m, load in zip(range(0, members, 8), loads):
        load.wait()

        def load_rows(t, carry, m=m):
            row = pl.multiple_of(t * 8, 8)
            place(x_ref, m, row, HALO + row)
            return carry

        lax.fori_loop(0, rows // 8, load_rows, 0)

    def wide(value):
        return jnp.concatenate([value] * (members // 8), axis=0)

    buffers = (one, two)
    for step in range(1, PASSES + 1):
        source, target = buffers[(step - 1) % 2], buffers[step % 2]
        first = HALO - PASSES + step
        count = total - 2 * first

        def advance(row, lines, source=source, target=target):
            middle = [source[row + i] for i in range(-1, lines + 1)]
            west = [pltpu.roll(m, 1, axis=1) for m in middle[1:-1]]
            east = [pltpu.roll(m, columns - 1, axis=1) for m in middle[1:-1]]
            for i in range(lines):
                target[row + i] = (
                    wide(coef[0, row + i]) * middle[i + 1]
                    + wide(coef[2, row + i]) * middle[i]
                    + wide(coef[1, row + i]) * west[i]
                    + wide(coef[3, row + i]) * (middle[i + 2] + east[i])
                )

        def sweep(t, carry, first=first, advance=advance):
            advance(first + LINES * t, LINES)
            return carry

        lax.fori_loop(0, count // LINES, sweep, 0)
        if count % LINES:
            advance(first + count // LINES * LINES, count % LINES)

    final = buffers[PASSES % 2]
    lane = lax.broadcasted_iota(jnp.int32, (members, 128), 1)

    def cut(t, carry):
        row = HALO + t * per
        at = pl.multiple_of(t * 128, 128)
        for m in range(0, members, 8):
            for h in range(columns // 128):
                lines = [final[row + i, m : m + 8, h * 128 : (h + 1) * 128] for i in range(per)]
                for j, piece in enumerate(swap_granules(lines, lane[:8], width)):
                    fields[h * per + j, m : m + 8, pl.ds(at, 128)] = piece
        return carry

    lax.fori_loop(0, rows // per, cut, 0)
    store = pltpu.make_async_copy(fields, out, out_sem)
    store.start()

    def look_at(b):
        index = jnp.broadcast_to(index_ref[b], (members, 128))
        low, high = index % 128, index // 128
        value = jnp.zeros((members, 128), F32)
        for t in range(cells // 128):
            part = fields[b, :, t * 128 : (t + 1) * 128]
            picked = jnp.take_along_axis(part, low, axis=1, mode="promise_in_bounds")
            value = jnp.where(high == t, picked, value)
        seen[b] = value

    def look(t, carry):
        for i in range(4):
            look_at(4 * t + i)
        return carry

    lax.fori_loop(0, blocks // 4, look, 0)
    store.wait()


def weight_kernel(partner_ref, own_ref, left_ref, right_ref, prec_ref, value_ref, high_ref, low_ref, stacked, innovation, mh, ml, zh, zl, fh, fl):
    blocks, chunk, nobs = own_ref.shape
    size = blocks * chunk
    for role, ref in enumerate((left_ref, own_ref, right_ref)):
        piece = ref[...].reshape(size, nobs)
        mean = jnp.sum(piece, axis=0, keepdims=True) * (1.0 / size)
        stacked[:, role * nobs : (role + 1) * nobs] = piece - mean
        innovation[:, role * nobs : (role + 1) * nobs] = value_ref[:, role * nobs : (role + 1) * nobs] - mean
    prec = prec_ref[...]
    spread = stacked[...]
    pull = jnp.sum(spread * (prec * innovation[...]), axis=1, keepdims=True)
    contract = (((1,), (1,)), ((), ()))
    gram = dot_split(split(spread * prec), split(spread), contract)
    eye = lax.broadcasted_iota(jnp.int32, (size, size), 0) == lax.broadcasted_iota(jnp.int32, (size, size), 1)
    gram = gram + jnp.where(eye, size - 1.0, 0.0)
    total = jnp.sum(jnp.sum(gram * gram, axis=0, keepdims=True), axis=1, keepdims=True)
    scale = lax.rsqrt(total)
    norm = jnp.sqrt(total)
    matrix = gram / norm

    def factor_of(product):
        diagonal = lax.broadcasted_iota(jnp.int32, (size, size), 0) == lax.broadcasted_iota(jnp.int32, (size, size), 1)
        return jnp.where(diagonal, 1.5, 0.0) - 0.5 * product

    mh[...], ml[...] = split(matrix)
    fh[...], fl[...] = split(factor_of(matrix))
    zh[...], zl[...] = fh[...], fl[...]
    mh[...], ml[...] = split(dot_split((mh[...], ml[...]), (fh[...], fl[...])))

    def iterate(step, carry):
        fh[...], fl[...] = split(factor_of(dot_split((zh[...], zl[...]), (mh[...], ml[...]))))
        mh[...], ml[...] = split(dot_split((mh[...], ml[...]), (fh[...], fl[...])))
        zh[...], zl[...] = split(dot_split((fh[...], fl[...]), (zh[...], zl[...])))
        return carry

    lax.fori_loop(0, NS_ITERS - 2, iterate, 0)
    fh[...], fl[...] = split(factor_of(dot_split((zh[...], zl[...]), (mh[...], ml[...]))))
    root = dot_split((fh[...], fl[...]), (zh[...], zl[...]))
    line = jnp.transpose(jnp.broadcast_to(pull, (size, 128)))[0:1]
    once = jnp.sum(root * line, axis=1, keepdims=True)
    twice = jnp.sum(root * once, axis=0, keepdims=True) / norm
    fh[...], fl[...] = split(jnp.sqrt((size - 1.0) * scale) * root + twice)
    for k in range(blocks):
        row = pl.multiple_of(partner_ref[k] * chunk, chunk)
        high_ref[k * chunk : (k + 1) * chunk, :] = fh[pl.ds(row, chunk), :]
        low_ref[k * chunk : (k + 1) * chunk, :] = fl[pl.ds(row, chunk), :]


def analysis_kernel(high_ref, low_ref, fields, *rest):
    outs, (ah, al) = rest[:-2], rest[-2:]
    blocks, chunk = fields.shape[:2]
    size = blocks * chunk
    total = fields[0]
    for k in range(1, blocks):
        total = total + fields[k]
    center = jnp.sum(total, axis=0, keepdims=True) * (1.0 / size)
    for k in range(blocks):
        row = k * chunk
        ah[row : row + chunk, :], al[row : row + chunk, :] = split(fields[k] - center)
    result = dot_split((high_ref[...], low_ref[...]), (ah[...], al[...]))
    for k in range(blocks):
        outs[k][...] = result[k * chunk : (k + 1) * chunk, :] + center


def assemble_kernel(blocks, partner_ref, *rest):
    pieces, (out_ref, fields, lines_ref) = rest[:blocks], rest[blocks:]
    members, rows, columns = out_ref.shape
    for k in range(blocks):
        fields[partner_ref[k]] = pieces[k][...]
    width = columns // blocks
    per = 128 // width
    lane = lax.broadcasted_iota(jnp.int32, (members, 128), 1)

    def join(t, carry):
        at = pl.multiple_of(t * 128, 128)
        for h in range(columns // 128):
            granules = [fields[h * per + j, :, pl.ds(at, 128)] for j in range(per)]
            for i, line in enumerate(swap_granules(granules, lane, width)):
                lines_ref[i, :, h * 128 : (h + 1) * 128] = line
        row = pl.multiple_of(t * per, 8)
        for m in range(0, members, 8):
            tile = lines_ref[:, m : m + 8, :]
            out_ref[m : m + 8, pl.ds(row, 8), :] = jnp.swapaxes(tile, 0, 1)
        return carry

    lax.fori_loop(0, rows // per, join, 0)


def cost(flops, moved):
    return pl.CostEstimate(flops=int(flops), bytes_accessed=int(moved), transcendentals=0)


def shape(dims, dtype=F32):
    return jax.ShapeDtypeStruct(dims, dtype)


PARAMS = pltpu.CompilerParams(vmem_limit_bytes=56 * 1024 * 1024)


def call_forecast(blocks, x, above, below, coefs, index):
    members, rows, columns = x.shape
    cells = rows * columns // blocks
    return pl.pallas_call(
        forecast_kernel,
        out_shape=[shape((blocks, members, cells)), shape((blocks, members, index.shape[2]))],
        in_specs=[HBM] + [VMEM] * 6,
        out_specs=[HBM, VMEM],
        scratch_shapes=[
            pltpu.VMEM((members, rows, columns), F32),
            pltpu.VMEM((blocks, members, cells), F32),
            pltpu.VMEM((rows + 2 * HALO, members, columns), F32),
            pltpu.VMEM((rows + 2 * HALO, members, columns), F32),
            pltpu.VMEM((4, rows + 2 * HALO, 8, columns), F32),
            pltpu.SemaphoreType.DMA((members // 8,)),
            pltpu.SemaphoreType.DMA,
        ],
        compiler_params=PARAMS,
        cost_estimate=cost(5e6, 5e6),
        name="forecast",
    )(x, above, below, *coefs, index)


def call_weight(partner, own, left, right, precision, values):
    blocks, members, nobs = own.shape
    size = blocks * members
    return pl.pallas_call(
        weight_kernel,
        out_shape=[shape((size, size), BF16)] * 2,
        in_specs=[SMEM] + [VMEM] * 5,
        out_specs=[VMEM] * 2,
        scratch_shapes=[pltpu.VMEM((size, 3 * nobs), F32), pltpu.VMEM((1, 3 * nobs), F32)]
        + [pltpu.VMEM((size, size), BF16)] * 6,
        compiler_params=PARAMS,
        cost_estimate=cost(5e9, 5e6),
        name="weight",
    )(partner, own, left, right, precision, values)


def call_analysis(high, low, fields):
    blocks, members, cells = fields.shape
    size = blocks * members
    whole = pl.BlockSpec((size, size), lambda i: (0, 0))
    return pl.pallas_call(
        analysis_kernel,
        grid=(PARTS,),
        out_shape=[shape((members, cells))] * blocks,
        in_specs=[whole, whole, pl.BlockSpec((blocks, members, cells // PARTS), lambda i: (0, 0, i))],
        out_specs=[pl.BlockSpec((members, cells // PARTS), lambda i: (0, i))] * blocks,
        scratch_shapes=[pltpu.VMEM((size, cells // PARTS), BF16)] * 2,
        compiler_params=PARAMS,
        cost_estimate=cost(1e9, 5e6),
        name="analysis",
    )(high, low, fields)


def call_assemble(partner, pieces, dims):
    members, _, columns = dims
    blocks = len(pieces)
    return pl.pallas_call(
        functools.partial(assemble_kernel, blocks),
        out_shape=shape(dims),
        in_specs=[SMEM] + [VMEM] * blocks,
        out_specs=VMEM,
        scratch_shapes=[pltpu.VMEM((blocks,) + pieces[0].shape, F32), pltpu.VMEM((8, members, columns), F32)],
        compiler_params=PARAMS,
        cost_estimate=cost(1e6, 5e6),
        name="assemble",
    )(partner, *pieces)


def body(
    starting_samples,
    transport_number_vertical,
    transport_number_horizontal,
    spreading_number,
    obs_value,
    obs_error,
    obs_index,
    loc_index,
    loc_table,
):
    blocks = lax.axis_size("mem")
    tiles = lax.axis_size("tile")
    members, rows, columns = starting_samples.shape
    me = lax.axis_index("mem")

    coefs = (transport_number_vertical, transport_number_horizontal, spreading_number)

    def edge(part):
        return jnp.concatenate([starting_samples[:, part]] + [c[None, part] for c in coefs], axis=0)

    up = [(i, (i + 1) % tiles) for i in range(tiles)]
    down = [(j, i) for i, j in up]
    above = lax.ppermute(edge(slice(rows - HALO, rows)), "tile", up)
    below = lax.ppermute(edge(slice(0, HALO)), "tile", down)

    fields, seen = call_forecast(blocks, starting_samples, above, below, coefs, obs_index[0][:, None, :])

    def swap(x, k):
        return lax.ppermute(x, "mem", [(i, i ^ k) for i in range(blocks)])

    ring = [(i, (i + 1) % blocks) for i in range(blocks)]
    seen, obs_value, obs_error, loc_index = lax.optimization_barrier((seen, obs_value, obs_error, loc_index))
    own = lax.all_to_all(seen, "mem", 0, 0)
    roles = (me + jnp.arange(3, dtype=jnp.int32) - 1) % blocks
    onehot = (loc_index[0][roles][:, :, None] == jnp.arange(loc_table.shape[1], dtype=jnp.int32)).astype(F32)
    precision = jnp.sum(onehot * loc_table[:, None, :], axis=2) / obs_error[0][roles]
    values = obs_value[0][roles]
    partner = jnp.bitwise_xor(me, jnp.arange(blocks, dtype=jnp.int32))
    own, precision, values, partner = lax.optimization_barrier((own, precision, values, partner))
    left = lax.ppermute(own, "mem", ring)
    right = lax.ppermute(own, "mem", [(j, i) for i, j in ring])
    fields = lax.all_to_all(fields, "mem", 0, 0)
    high, low = call_weight(partner, own, left, right, precision.reshape(1, -1), values.reshape(1, -1))
    result = call_analysis(high, low, fields)
    back = {0: result[0]}
    for k in range(blocks - 1, 0, -1):
        back[k] = swap(result[k], k)
    return call_assemble(partner, [back[k] for k in range(blocks)], (members, rows, columns))


def solution(mesh):
    in_specs = (
        P("mem", "tile", None),
        P("tile", None),
        P("tile", None),
        P("tile", None),
        P("tile", None, None),
        P("tile", None, None),
        P("tile", None, None),
        P("tile", None, None),
        P(),
    )
    out_specs = P("mem", "tile", None)
    return jax.shard_map(body, mesh=mesh, in_specs=in_specs, out_specs=out_specs, check_vma=False)
```

```python
import functools

import jax
import jax.numpy as jnp
from jax import lax
from jax.experimental import pallas as pl
from jax.experimental.pallas import tpu as pltpu
from jax.sharding import PartitionSpec as P


PASSES = 6
NS_ITERS = 8
HALO = 8
LINES = 36
PARTS = 2
STEPS = 2
F32 = jnp.float32
BF16 = jnp.bfloat16
VMEM = pl.BlockSpec(memory_space=pltpu.VMEM)
SMEM = pl.BlockSpec(memory_space=pltpu.SMEM)
HBM = pl.BlockSpec(memory_space=pltpu.HBM)


def split(x):
    high = x.astype(BF16)
    return high, (x - high.astype(F32)).astype(BF16)


def dot_split(a, b, dims=(((1,), (0,)), ((), ()))):
    (ah, al), (bh, bl) = a, b
    dot = functools.partial(lax.dot_general, dimension_numbers=dims, preferred_element_type=F32)
    return dot(ah, bh) + (dot(ah, bl) + dot(al, bh))


def swap_granules(rows, lane, width):
    count = len(rows)
    rows = list(rows)
    step = count // 2
    while step:
        odd = (lane // (width * step)) % 2 == 1
        for i in range(count):
            if i & step:
                continue
            a, b = rows[i], rows[i + step]
            rows[i] = jnp.where(odd, pltpu.roll(b, width * step, axis=1), a)
            rows[i + step] = jnp.where(odd, b, pltpu.roll(a, 128 - width * step, axis=1))
        step //= 2
    return rows


def forecast_kernel(x_hbm, up_ref, down_ref, av_ref, ah_ref, sp_ref, index_ref, *rest):
    out, seen, x_ref, fields, one, two, coef, in_sems, out_sem = rest
    blocks = fields.shape[0]
    members, rows, columns = x_ref.shape
    loads = []
    for m in range(0, members, 8):
        loads.append(pltpu.make_async_copy(x_hbm.at[pl.ds(m, 8)], x_ref.at[pl.ds(m, 8)], in_sems.at[m // 8]))
        loads[-1].start()
    total = rows + 2 * HALO
    width = columns // blocks
    per = 128 // width
    cells = rows * width

    def place(source, member, row, target):
        tile = source[pl.ds(member, 8), pl.ds(row, 8), :]
        one[pl.ds(target, 8), pl.ds(member, 8), :] = jnp.swapaxes(tile, 0, 1)

    for m in range(0, members, 8):
        place(up_ref, m, 0, 0)
        place(down_ref, m, 0, HALO + rows)

    def spread_coef(av, ah, sp, target):
        for n, value in enumerate((1.0 - av - ah - 4.0 * sp, av + sp, ah + sp, sp)):
            for i in range(8):
                coef[n, target + i] = jnp.broadcast_to(value[i : i + 1], (8, columns))

    spread_coef(up_ref[members], up_ref[members + 1], up_ref[members + 2], 0)
    spread_coef(down_ref[members], down_ref[members + 1], down_ref[members + 2], HALO + rows)

    def coef_rows(t, carry):
        row = pl.multiple_of(t * 8, 8)
        spread_coef(av_ref[pl.ds(row, 8), :], ah_ref[pl.ds(row, 8), :], sp_ref[pl.ds(row, 8), :], HALO + row)
        return carry

    lax.fori_loop(0, rows // 8, coef_rows, 0)
    for m, load in zip(range(0, members, 8), loads):
        load.wait()

        def load_rows(t, carry, m=m):
            row = pl.multiple_of(t * 8, 8)
            place(x_ref, m, row, HALO + row)
            return carry

        lax.fori_loop(0, rows // 8, load_rows, 0)

    def wide(value):
        return jnp.concatenate([value] * (members // 8), axis=0)

    buffers = (one, two)
    for step in range(1, PASSES + 1):
        source, target = buffers[(step - 1) % 2], buffers[step % 2]
        first = HALO - PASSES + step
        count = total - 2 * first

        def advance(row, lines, source=source, target=target):
            middle = [source[row + i] for i in range(-1, lines + 1)]
            west = [pltpu.roll(m, 1, axis=1) for m in middle[1:-1]]
            east = [pltpu.roll(m, columns - 1, axis=1) for m in middle[1:-1]]
            for i in range(lines):
                target[row + i] = (
                    wide(coef[0, row + i]) * middle[i + 1]
                    + wide(coef[2, row + i]) * middle[i]
                    + wide(coef[1, row + i]) * west[i]
                    + wide(coef[3, row + i]) * (middle[i + 2] + east[i])
                )

        def sweep(t, carry, first=first, advance=advance):
            advance(first + LINES * t, LINES)
            return carry

        lax.fori_loop(0, count // LINES, sweep, 0)
        if count % LINES:
            advance(first + count // LINES * LINES, count % LINES)

    final = buffers[PASSES % 2]
    tiles = columns // 128
    lane = lax.broadcasted_iota(jnp.int32, (tiles * members, 128), 1)

    def cut(t, carry):
        row = HALO + t * per
        at = pl.multiple_of(t * 128, 128)
        lines = []
        for i in range(per):
            parts = [final[row + i, :, h * 128 : (h + 1) * 128] for h in range(tiles)]
            lines.append(jnp.concatenate(parts, axis=0))
        for j, piece in enumerate(swap_granules(lines, lane, width)):
            for h in range(tiles):
                fields[h * per + j, :, pl.ds(at, 128)] = piece[h * members : (h + 1) * members]
        return carry

    lax.fori_loop(0, rows // per, cut, 0)
    store = pltpu.make_async_copy(fields, out, out_sem)
    store.start()

    def look_at(b):
        index = jnp.broadcast_to(index_ref[b], (members, 128))
        low, high = index % 128, index // 128
        value = jnp.zeros((members, 128), F32)
        for t in range(cells // 128):
            part = fields[b, :, t * 128 : (t + 1) * 128]
            picked = jnp.take_along_axis(part, low, axis=1, mode="promise_in_bounds")
            value = jnp.where(high == t, picked, value)
        seen[b] = value

    def look(t, carry):
        for i in range(4):
            look_at(4 * t + i)
        return carry

    lax.fori_loop(0, blocks // 4, look, 0)
    store.wait()


def weight_kernel(partner_ref, own_ref, left_ref, right_ref, prec_ref, value_ref, high_ref, low_ref, stacked, innovation, mh, ml, zh, zl, fh, fl):
    blocks, chunk, nobs = own_ref.shape
    size = blocks * chunk
    for role, ref in enumerate((left_ref, own_ref, right_ref)):
        piece = ref[...].reshape(size, nobs)
        mean = jnp.sum(piece, axis=0, keepdims=True) * (1.0 / size)
        stacked[:, role * nobs : (role + 1) * nobs] = piece - mean
        innovation[:, role * nobs : (role + 1) * nobs] = value_ref[:, role * nobs : (role + 1) * nobs] - mean
    prec = prec_ref[...]
    spread = stacked[...]
    pull = jnp.sum(spread * (prec * innovation[...]), axis=1, keepdims=True)
    contract = (((1,), (1,)), ((), ()))
    gram = dot_split(split(spread * prec), split(spread), contract)
    eye = lax.broadcasted_iota(jnp.int32, (size, size), 0) == lax.broadcasted_iota(jnp.int32, (size, size), 1)
    gram = gram + jnp.where(eye, size - 1.0, 0.0)
    total = jnp.sum(jnp.sum(gram * gram, axis=0, keepdims=True), axis=1, keepdims=True)
    scale = lax.rsqrt(total)
    norm = jnp.sqrt(total)
    matrix = gram / norm

    def factor_of(product):
        diagonal = lax.broadcasted_iota(jnp.int32, (size, size), 0) == lax.broadcasted_iota(jnp.int32, (size, size), 1)
        return jnp.where(diagonal, 1.5, 0.0) - 0.5 * product

    mh[...], ml[...] = split(matrix)
    fh[...], fl[...] = split(factor_of(matrix))
    zh[...], zl[...] = fh[...], fl[...]
    mh[...], ml[...] = split(dot_split((mh[...], ml[...]), (fh[...], fl[...])))

    def iterate(step, carry):
        fh[...], fl[...] = split(factor_of(dot_split((zh[...], zl[...]), (mh[...], ml[...]))))
        mh[...], ml[...] = split(dot_split((mh[...], ml[...]), (fh[...], fl[...])))
        zh[...], zl[...] = split(dot_split((fh[...], fl[...]), (zh[...], zl[...])))
        return carry

    lax.fori_loop(0, NS_ITERS - 2, iterate, 0)
    fh[...], fl[...] = split(factor_of(dot_split((zh[...], zl[...]), (mh[...], ml[...]))))
    root = dot_split((fh[...], fl[...]), (zh[...], zl[...]))
    line = jnp.transpose(jnp.broadcast_to(pull, (size, 128)))[0:1]
    once = jnp.sum(root * line, axis=1, keepdims=True)
    twice = jnp.sum(root * once, axis=0, keepdims=True) / norm
    fh[...], fl[...] = split(jnp.sqrt((size - 1.0) * scale) * root + twice)
    for k in range(blocks):
        row = pl.multiple_of(partner_ref[k] * chunk, chunk)
        high_ref[k * chunk : (k + 1) * chunk, :] = fh[pl.ds(row, chunk), :]
        low_ref[k * chunk : (k + 1) * chunk, :] = fl[pl.ds(row, chunk), :]


def analysis_kernel(high_ref, low_ref, fields, *rest):
    outs, (ah, al) = rest[:-2], rest[-2:]
    blocks, chunk = fields.shape[:2]
    size = blocks * chunk
    total = fields[0]
    for k in range(1, blocks):
        total = total + fields[k]
    center = jnp.sum(total, axis=0, keepdims=True) * (1.0 / size)
    for k in range(blocks):
        row = k * chunk
        ah[row : row + chunk, :], al[row : row + chunk, :] = split(fields[k] - center)
    result = dot_split((high_ref[...], low_ref[...]), (ah[...], al[...]))
    for k in range(blocks):
        outs[k][...] = result[k * chunk : (k + 1) * chunk, :] + center


def assemble_kernel(half, place_ref, *rest):
    pieces, (out_ref, fields) = rest[:half], rest[-2:]
    members, rows, columns = out_ref.shape
    width = columns // half
    per = 128 // width
    groups = rows // per
    for k in range(half):
        fields[place_ref[k + 1]] = pieces[k][...]
    lane = lax.broadcasted_iota(jnp.int32, (groups * members, 128), 1)
    for h in range(columns // 128):
        granules = []
        for j in range(per):
            parts = [fields[h * per + j, :, t * 128 : (t + 1) * 128] for t in range(groups)]
            granules.append(jnp.concatenate(parts, axis=0))
        lines = swap_granules(granules, lane, width)
        for t in range(groups):
            for m in range(0, members, 8):
                at = t * members + m
                block = jnp.concatenate([line[at : at + 8][None] for line in lines], axis=0)
                row = t * per
                out_ref[m : m + 8, row : row + per, h * 128 : (h + 1) * 128] = jnp.swapaxes(block, 0, 1)


def cost(flops, moved):
    return pl.CostEstimate(flops=int(flops), bytes_accessed=int(moved), transcendentals=0)


def shape(dims, dtype=F32):
    return jax.ShapeDtypeStruct(dims, dtype)


PARAMS = pltpu.CompilerParams(vmem_limit_bytes=56 * 1024 * 1024)


def call_forecast(blocks, x, above, below, coefs, index):
    members, rows, columns = x.shape
    cells = rows * columns // blocks
    return pl.pallas_call(
        forecast_kernel,
        out_shape=[shape((blocks, members, cells)), shape((blocks, members, index.shape[2]))],
        in_specs=[HBM] + [VMEM] * 6,
        out_specs=[HBM, VMEM],
        scratch_shapes=[
            pltpu.VMEM((members, rows, columns), F32),
            pltpu.VMEM((blocks, members, cells), F32),
            pltpu.VMEM((rows + 2 * HALO, members, columns), F32),
            pltpu.VMEM((rows + 2 * HALO, members, columns), F32),
            pltpu.VMEM((4, rows + 2 * HALO, 8, columns), F32),
            pltpu.SemaphoreType.DMA((members // 8,)),
            pltpu.SemaphoreType.DMA,
        ],
        compiler_params=PARAMS,
        cost_estimate=cost(5e6, 5e6),
        name="forecast",
    )(x, above, below, *coefs, index)


def call_weight(partner, own, left, right, precision, values):
    blocks, members, nobs = own.shape
    size = blocks * members
    return pl.pallas_call(
        weight_kernel,
        out_shape=[shape((size, size), BF16)] * 2,
        in_specs=[SMEM] + [VMEM] * 5,
        out_specs=[VMEM] * 2,
        scratch_shapes=[pltpu.VMEM((size, 3 * nobs), F32), pltpu.VMEM((1, 3 * nobs), F32)]
        + [pltpu.VMEM((size, size), BF16)] * 6,
        compiler_params=pltpu.CompilerParams(vmem_limit_bytes=63 * 1024 * 1024),
        cost_estimate=cost(5e9, 5e6),
        name="weight",
    )(partner, own, left, right, precision, values)


def call_analysis(high, low, fields):
    blocks, members, cells = fields.shape
    size = blocks * members
    whole = pl.BlockSpec((size, size), lambda i: (0, 0))
    return pl.pallas_call(
        analysis_kernel,
        grid=(PARTS,),
        out_shape=[shape((members, cells))] * blocks,
        in_specs=[whole, whole, pl.BlockSpec((blocks, members, cells // PARTS), lambda i: (0, 0, i))],
        out_specs=[pl.BlockSpec((members, cells // PARTS), lambda i: (0, i))] * blocks,
        scratch_shapes=[pltpu.VMEM((size, cells // PARTS), BF16)] * 2,
        compiler_params=PARAMS,
        cost_estimate=cost(1e9, 5e6),
        name="analysis",
    )(high, low, fields)


def call_assemble(place, pieces, dims, before=None):
    members, rows, columns = dims
    half = len(pieces)
    steps = STEPS
    piece = pl.BlockSpec((members, pieces[0].shape[1] // steps), lambda i, place: (0, i))
    extra = [] if before is None else [before]
    return pl.pallas_call(
        functools.partial(assemble_kernel, half),
        out_shape=shape(dims),
        grid_spec=pltpu.PrefetchScalarGridSpec(
            num_scalar_prefetch=1,
            grid=(steps,),
            in_specs=[piece] * half + [HBM] * len(extra),
            out_specs=pl.BlockSpec((members, rows // steps, columns // 2), lambda i, place: (0, i, place[0])),
            scratch_shapes=[pltpu.VMEM((half, members, pieces[0].shape[1] // steps), F32)],
        ),
        input_output_aliases={half + 1: 0} if extra else {},
        compiler_params=PARAMS,
        cost_estimate=cost(1e9, 5e6),
        name="assemble",
    )(place, *pieces, *extra)


def body(
    starting_samples,
    transport_number_vertical,
    transport_number_horizontal,
    spreading_number,
    obs_value,
    obs_error,
    obs_index,
    loc_index,
    loc_table,
):
    blocks = lax.axis_size("mem")
    tiles = lax.axis_size("tile")
    members, rows, columns = starting_samples.shape
    me = lax.axis_index("mem")

    coefs = (transport_number_vertical, transport_number_horizontal, spreading_number)

    def edge(part):
        return jnp.concatenate([starting_samples[:, part]] + [c[None, part] for c in coefs], axis=0)

    up = [(i, (i + 1) % tiles) for i in range(tiles)]
    down = [(j, i) for i, j in up]
    above = lax.ppermute(edge(slice(rows - HALO, rows)), "tile", up)
    below = lax.ppermute(edge(slice(0, HALO)), "tile", down)

    fields, seen = call_forecast(blocks, starting_samples, above, below, coefs, obs_index[0][:, None, :])

    def swap(x, k):
        return lax.ppermute(x, "mem", [(i, i ^ k) for i in range(blocks)])

    ring = [(i, (i + 1) % blocks) for i in range(blocks)]
    seen, obs_value, obs_error, loc_index = lax.optimization_barrier((seen, obs_value, obs_error, loc_index))
    own = lax.all_to_all(seen, "mem", 0, 0)
    roles = (me + jnp.arange(3, dtype=jnp.int32) - 1) % blocks
    onehot = (loc_index[0][roles][:, :, None] == jnp.arange(loc_table.shape[1], dtype=jnp.int32)).astype(F32)
    precision = jnp.sum(onehot * loc_table[:, None, :], axis=2) / obs_error[0][roles]
    values = obs_value[0][roles]
    partner = jnp.bitwise_xor(me, jnp.arange(blocks, dtype=jnp.int32))
    own, precision, values, partner = lax.optimization_barrier((own, precision, values, partner))
    left = lax.ppermute(own, "mem", ring)
    right = lax.ppermute(own, "mem", [(j, i) for i, j in ring])
    fields = lax.all_to_all(fields, "mem", 0, 0)
    high, low = call_weight(partner, own, left, right, precision.reshape(1, -1), values.reshape(1, -1))
    result = call_analysis(high, low, fields)
    half = blocks // 2
    back = {0: result[0]}
    for k in range(half + 3 * half // 4, blocks):
        back[k] = swap(result[k], k)
    for k in range(half - 1, 0, -1):
        back[k] = swap(result[k], k)
    for k in range(half, half + 3 * half // 4):
        back[k] = swap(result[k], k)
    side = me // half
    local = partner[:half] % half
    dims = (members, rows, columns)
    out = call_assemble(jnp.concatenate([side[None], local]), [back[k] for k in range(half)], dims)
    there = jnp.concatenate([1 - side[None], local])
    return call_assemble(there, [back[k] for k in range(half, blocks)], dims, out)


def solution(mesh):
    in_specs = (
        P("mem", "tile", None),
        P("tile", None),
        P("tile", None),
        P("tile", None),
        P("tile", None, None),
        P("tile", None, None),
        P("tile", None, None),
        P("tile", None, None),
        P(),
    )
    out_specs = P("mem", "tile", None)
    return jax.shard_map(body, mesh=mesh, in_specs=in_specs, out_specs=out_specs, check_vma=False)
```
